32 devices in a mesh: dp: 16 (over z, x, core), outer: 2 (over y).
Axes of the slice: x: 2, y: 2, z: 4, core: 2. Of those that a mesh axis runs over, the one named last changes fastest.
Arguments:
- images: bfloat16 [2048, 1024], P('dp'), may hold values from -8 to 8
- texts: bfloat16 [2048, 1024], P(('dp', 'outer')), may hold values from -8 to 8
- logit_scale: float32 [1], replicated, may hold values from 70 to 100
Outputs:
- image_loss: float32 [2048], P(('dp', 'outer'))
- text_loss: float32 [2048], P(('dp', 'outer'))
The draws below stay inside these ranges and needn't reach their ends.
All inputs are finite; a program needn't handle non-finite values.
Results may differ from the reference program's by a relative error of at most 0.003.
Values may be sent and summed in bfloat16 or wider, within the bound.
A program may use at most 64 MiB of HBM per device.

```python
import math
import jax
import jax.numpy as jnp
from jax import lax

D = 1024
BATCH = 2048


def raw_features(key, salt):
    normal_draw = jax.random.normal(jax.random.fold_in(key, salt), (BATCH, D), jnp.float32)
    return jnp.clip(normal_draw, -8.0, 8.0)


def draw_images(key, part):
    return raw_features(key, 1).astype(jnp.bfloat16)


def draw_texts(key, part):
    own_texts = raw_features(key, 2)
    return own_texts.astype(jnp.bfloat16)


def draw_logit_scale(key, part):
    return jax.random.uniform(jax.random.fold_in(key, 3), (1,), jnp.float32, 70.0, 100.0)


def setup_inputs(seed: int = 0) -> dict:
    streams_of = jax.random.split(jax.random.key(seed), 4)
    images = draw_images(jax.random.fold_in(streams_of[3], 71), 0)
    texts = draw_texts(jax.random.fold_in(streams_of[3], 71), 0)
    logit_scale = draw_logit_scale(jax.random.fold_in(streams_of[3], 71), 0)
    return dict(images=images, texts=texts, logit_scale=logit_scale)


def normalise(features):
    widened = features.astype(jnp.float32)
    return (widened * lax.rsqrt(lax.optimization_barrier(jnp.sum(widened * widened, axis=1, keepdims=True)) + 1.0)).astype(jnp.bfloat16)

def reference(images, texts, logit_scale):
    image_unit = normalise(images)
    text_unit = normalise(texts)
    factor = logit_scale[0]
    block_size = math.gcd(BATCH, 1024)
    text_blocks = text_unit.reshape(BATCH // block_size, block_size, D)

    def absorb_block(states, text_block):
        row_peak, row_total = states
        scores = jnp.einsum('id,jd->ij', image_unit, text_block, preferred_element_type=jnp.float32) * factor
        col_peak = lax.optimization_barrier(jnp.max(scores, axis=0))
        col_lse = col_peak + jnp.log(lax.optimization_barrier(jnp.sum(jnp.exp(scores - col_peak), axis=0)))
        new_peak = jnp.maximum(row_peak, lax.optimization_barrier(jnp.max(scores, axis=1)))
        row_total = row_total * jnp.exp(row_peak - new_peak) + lax.optimization_barrier(jnp.sum(jnp.exp(scores - new_peak[:, None]), axis=1))
        return ((new_peak, row_total), col_lse)
    initial = (jnp.full((BATCH,), -1e+30, jnp.float32), jnp.zeros((BATCH,), jnp.float32))
    (row_peak, row_total), col_lse = lax.scan(absorb_block, initial, text_blocks)
    diagonal = lax.optimization_barrier(jnp.sum(image_unit.astype(jnp.float32) * text_unit.astype(jnp.float32), axis=1)) * factor
    image_loss = row_peak + jnp.log(row_total) - diagonal
    text_loss = col_lse.reshape(BATCH) - diagonal
    return (image_loss, text_loss)
```

```python
import functools

import jax
import jax.numpy as jnp
from jax import lax
from jax.experimental import pallas as pl
from jax.experimental.pallas import tpu as pltpu
from jax.sharding import PartitionSpec as P

MESH = pl.DeviceIdType.MESH
TEXT_CHUNKS = 2
IMAGE_CHUNKS = 2
LANES = 128
VMEM_BYTES = 66920448


def lane_partial(rows_a, rows_b):
    product = rows_a.astype(jnp.float32) * rows_b.astype(jnp.float32)
    total = product[:, :LANES]
    for start in range(LANES, product.shape[1], LANES):
        total = total + product[:, start : start + LANES]
    return total


def kernel(
    dims, scale_ref, img_hbm, txt_hbm, out,
    im, tx, im_scale, scores, st_i, st_t, got_i, got_t,
    load_sem, own_send, own_recv, tz_send, iz_send, x_send, y_send, d_send, tx_recv, im_recv,
    si_send, st_send, si_recv, st_recv,
):
    planes_i, planes_t, rows = dims
    t_piece, i_piece = rows // TEXT_CHUNKS, rows // IMAGE_CHUNKS
    me, y = lax.axis_index("dp"), lax.axis_index("outer")
    c, x, z = me % 2, (me // 2) % 2, me // 4
    p, group = z % planes_i, z // planes_i

    def at(zz, xx, cc, yy):
        return ((zz * 2 + xx) * 2 + cc, yy)

    def image_plane(pp):
        return group * planes_i + pp

    def text_plane(q):
        return q * planes_i + p

    def im_at(pp, k, h, ch):
        start = ((pp * 2 + k) * 2 + h) * rows + ch * i_piece
        return im.at[pl.ds(pl.multiple_of(start, i_piece), i_piece)]

    def im_shard(k):
        return im.at[pl.ds(pl.multiple_of((p * 2 + k) * 2 * rows, 2 * rows), 2 * rows)]

    def tx_at(q, xs, ch):
        return tx.at[pl.ds(pl.multiple_of((q * 2 + xs) * rows + ch * t_piece, t_piece), t_piece)]

    def tx_shard(xs):
        return tx.at[pl.ds(pl.multiple_of((group * 2 + xs) * rows, rows), rows)]

    def rc(src, dst, ss, rs, dev):
        return pltpu.make_async_remote_copy(
            src_ref=src, dst_ref=dst, send_sem=ss, recv_sem=rs, device_id=dev, device_id_type=MESH
        )

    img_load = pltpu.make_async_copy(img_hbm, im_shard(c), load_sem.at[0])
    txt_load = pltpu.make_async_copy(txt_hbm, tx_shard(x), load_sem.at[1])
    img_load.start()
    txt_load.start()

    barrier = pltpu.get_barrier_semaphore()
    partners = [at(text_plane((group + d) % planes_t), x, c, y) for d in range(1, planes_t)]
    partners += [at(image_plane((p + d) % planes_i), x, c, y) for d in range(1, planes_i)]
    partners += [at(z, 1 - x, c, y), at(z, x, c, 1 - y), at(z, x, 1 - c, y)]
    for dev in partners:
        pl.semaphore_signal(barrier, inc=1, device_id=dev, device_id_type=MESH)
    img_load.wait()
    txt_load.wait()
    pl.semaphore_wait(barrier, len(partners))

    def text_z(d, ch):
        return rc(tx_at(group, x, ch), tx_at(group, x, ch), tz_send.at[d - 1, ch],
                  tx_recv.at[group, x, ch], at(text_plane((group + d) % planes_t), x, c, y))

    def text_x_own(xs):
        return rc(tx_shard(xs), tx_shard(xs), own_send.at[0], own_recv.at[0], at(z, 1 - x, c, y))

    def text_x(d, xs, ch):
        q = (group + d) % planes_t
        return rc(tx_at(q, xs, ch), tx_at(q, xs, ch), x_send.at[d - 1, ch],
                  tx_recv.at[q, xs, ch], at(z, 1 - x, c, y))

    def image_z(d, ch):
        return rc(im_at(p, c, y, ch), im_at(p, c, y, ch), iz_send.at[d - 1, ch],
                  im_recv.at[p, c, y, ch], at(image_plane((p + d) % planes_i), x, c, y))

    def image_y(d, h, ch):
        pp = (p + d) % planes_i
        return rc(im_at(pp, c, h, ch), im_at(pp, c, h, ch), y_send.at[d - 1, ch],
                  im_recv.at[pp, c, h, ch], at(z, x, c, 1 - y))

    def image_d_own(k):
        return rc(im_shard(k), im_shard(k), own_send.at[1], own_recv.at[1], at(z, x, 1 - c, y))

    def image_d(d, k, h, ch):
        pp = (p + d) % planes_i
        return rc(im_at(pp, k, h, ch), im_at(pp, k, h, ch), d_send.at[d - 1, h, ch],
                  im_recv.at[pp, k, h, ch], at(z, x, 1 - c, y))

    for ch in range(IMAGE_CHUNKS):
        for d in range(1, planes_i):
            image_z(d, ch).start()
    for ch in range(TEXT_CHUNKS):
        for d in range(1, planes_t):
            text_z(d, ch).start()
    text_x_own(x).start()
    image_d_own(c).start()

    def pass_text(ch):
        for d in range(1, planes_t):
            copy = text_x(d, x, ch)
            copy.wait_recv()
            copy.start()

    def pass_image(ch):
        for d in range(1, planes_i):
            copy = image_y(d, y, ch)
            copy.wait_recv()
            copy.start()
            image_d(d, c, y, ch).start()

    def pass_to_core(ch):
        for d in range(1, planes_i):
            image_y(d, 1 - y, ch).wait_recv()
            image_d(d, c, 1 - y, ch).start()

    per = TEXT_CHUNKS // IMAGE_CHUNKS
    inner = p != group % 2

    @pl.when(inner)
    def _():
        for ch in range(IMAGE_CHUNKS):
            pass_image(ch)
        for ch in range(TEXT_CHUNKS):
            pass_text(ch)
            if ch < IMAGE_CHUNKS:
                pass_to_core(ch)

    @pl.when(jnp.logical_not(inner))
    def _():
        for ch in range(TEXT_CHUNKS):
            pass_text(ch)
            if ch % per == per - 1:
                pass_image(ch // per)
        for ch in range(IMAGE_CHUNKS):
            pass_to_core(ch)

    factor = scale_ref[0]
    wide, deep = 2 * rows, 4 * rows

    def im_rows(pp):
        return pl.ds(pl.multiple_of(pp * deep, deep), deep)

    def scale_images(pp):
        images = im[im_rows(pp), :]
        total = jnp.sum(lane_partial(images, images), axis=1, keepdims=True)
        im_scale[im_rows(pp), :] = jnp.broadcast_to(lax.rsqrt(total + 1.0) * factor, (deep, wide))

    def read_texts(q):
        texts = tx[pl.ds(pl.multiple_of(q * wide, wide), wide), :]
        total = jnp.sum(jnp.transpose(lane_partial(texts, texts)), axis=0, keepdims=True)
        return texts, lax.rsqrt(total + 1.0)

    def score(pp, q, texts, text_scale):
        block = lax.dot_general(
            im[im_rows(pp), :], texts, (((1,), (1,)), ((), ())), preferred_element_type=jnp.float32
        )
        block = block * im_scale[im_rows(pp), :] * text_scale
        scores[im_rows(pp), pl.ds(pl.multiple_of(q * wide, wide), wide)] = block

    def text_stats(q):
        block = scores[:, pl.ds(pl.multiple_of(q * wide, wide), wide)]
        peak = jnp.max(block, axis=0, keepdims=True)
        lse = peak + jnp.log(jnp.sum(jnp.exp(block - peak), axis=0, keepdims=True))
        st_t[q] = jnp.broadcast_to(lse, (8, wide))

    def stat_t(q, xs):
        return rc(st_t.at[q], got_t.at[group * 2 + x], st_send.at[q, xs],
                  st_recv.at[group * 2 + x], at(text_plane(q), xs, c, y))

    def stat_i(pp, k, h):
        slot = (p * 2 + y) * 2 + c
        return rc(st_i.at[pp * 2 + k], got_i.at[slot], si_send.at[pp, k, h],
                  si_recv.at[slot], at(image_plane(pp), x, k, h))

    t_pairs = [(q, xs) for q in range(planes_t) for xs in range(2)]
    i_triples = [(pp, k, h) for pp in range(planes_i) for k in range(2) for h in range(2)]

    def t_self(q, xs):
        return jnp.logical_and(text_plane(q) == z, xs == x)

    def i_self(pp, k, h):
        return (pp * 2 + k) * 2 + h == (p * 2 + c) * 2 + y

    def send_text_stats(q, xs):
        mine = t_self(q, xs)

        @pl.when(jnp.logical_not(mine))
        def _():
            stat_t(q, xs).start()

        @pl.when(mine)
        def _():
            got_t[group * 2 + x] = st_t[q]

    image_d_own(1 - c).wait_recv()
    scale_images(p)
    text_x_own(1 - x).wait_recv()
    own_texts = read_texts(group)
    score(p, group, *own_texts)
    for d in range(1, planes_i):
        for h in range(2):
            for ch in range(IMAGE_CHUNKS):
                image_d(d, 1 - c, h, ch).wait_recv()
        pp = (p + d) % planes_i
        scale_images(pp)
        score(pp, group, *own_texts)
    text_stats(group)
    for xs in range(2):
        send_text_stats(group, xs)
    for d in range(1, planes_t):
        for ch in range(TEXT_CHUNKS):
            text_x(d, 1 - x, ch).wait_recv()
        q = (group + d) % planes_t
        texts = read_texts(q)
        for pp in range(planes_i):
            score(pp, q, *texts)
        text_stats(q)
        for xs in range(2):
            send_text_stats(q, xs)

    for s in range(planes_i * 2):
        block = scores[pl.ds(s * 2 * rows, 2 * rows), :]
        peak = jnp.max(block, axis=1, keepdims=True)
        lse = peak + jnp.log(jnp.sum(jnp.exp(block - peak), axis=1, keepdims=True))
        st_i[s] = jnp.transpose(jnp.broadcast_to(lse, (2 * rows, LANES)))[:8, :]

    for pp, k, h in i_triples:
        mine = i_self(pp, k, h)

        @pl.when(jnp.logical_not(mine))
        def _():
            stat_i(pp, k, h).start()

        @pl.when(mine)
        def _():
            got_i[(p * 2 + y) * 2 + c] = st_i[pp * 2 + k]

    own_img = im[pl.ds(pl.multiple_of(((p * 2 + c) * 2 + y) * rows, rows), rows), :]
    own_txt = tx[pl.ds(pl.multiple_of((group * 2 + x) * rows, rows), rows), :]

    def row_sum(a, b):
        return jnp.sum(jnp.transpose(lane_partial(a, b)), axis=0, keepdims=True)

    diagonal = (
        row_sum(own_img, own_txt)
        * lax.rsqrt(row_sum(own_img, own_img) + 1.0)
        * lax.rsqrt(row_sum(own_txt, own_txt) + 1.0)
        * factor
    )

    text_x_own(x).wait_send()
    image_d_own(c).wait_send()
    for ch in range(TEXT_CHUNKS):
        for d in range(1, planes_t):
            text_z(d, ch).wait_send()
            text_x(d, x, ch).wait_send()
    for ch in range(IMAGE_CHUNKS):
        for d in range(1, planes_i):
            image_z(d, ch).wait_send()
            image_y(d, y, ch).wait_send()
            for h in range(2):
                image_d(d, c, h, ch).wait_send()

    def merge(got, count):
        parts = [got[s][0:1, :] for s in range(count)]
        peak = functools.reduce(jnp.maximum, parts)
        total = functools.reduce(jnp.add, [jnp.exp(part - peak) for part in parts])
        return peak + jnp.log(total)

    for s in range(planes_i * 4):

        @pl.when(s != (p * 2 + y) * 2 + c)
        def _():
            rc(st_i.at[0], got_i.at[s], si_send.at[0, 0, 0], si_recv.at[s], at(z, x, 1 - c, y)).wait_recv()

    lse = merge(got_i, planes_i * 4)
    out[0:1, :] = jnp.where(y == 0, lse[:, :rows], lse[:, rows:]) - diagonal

    for s in range(planes_t * 2):

        @pl.when(s != group * 2 + x)
        def _():
            rc(st_t.at[0], got_t.at[s], st_send.at[0, 0], st_recv.at[s], at(z, x, 1 - c, y)).wait_recv()

    lse = merge(got_t, planes_t * 2)
    out[1:2, :] = jnp.where(x == 0, lse[:, :rows], lse[:, rows:]) - diagonal

    for q, xs in t_pairs:

        @pl.when(jnp.logical_not(t_self(q, xs)))
        def _():
            stat_t(q, xs).wait_send()

    for pp, k, h in i_triples:

        @pl.when(jnp.logical_not(i_self(pp, k, h)))
        def _():
            stat_i(pp, k, h).wait_send()


def on_device(planes_i, planes_t, images, texts, logit_scale):
    rows, width = texts.shape
    dma = pltpu.SemaphoreType.DMA
    f32 = jnp.float32
    losses = pl.pallas_call(
        functools.partial(kernel, (planes_i, planes_t, rows)),
        out_shape=pltpu.VMEM((2, rows), f32),
        in_specs=[
            pl.BlockSpec(memory_space=pltpu.SMEM),
            pl.BlockSpec(memory_space=pltpu.HBM),
            pl.BlockSpec(memory_space=pltpu.HBM),
        ],
        out_specs=pl.BlockSpec(memory_space=pltpu.VMEM),
        scratch_shapes=[
            pltpu.VMEM((planes_i * 4 * rows, width), images.dtype),
            pltpu.VMEM((planes_t * 2 * rows, width), texts.dtype),
            pltpu.VMEM((planes_i * 4 * rows, 2 * rows), f32),
            pltpu.VMEM((planes_i * 4 * rows, planes_t * 2 * rows), f32),
            pltpu.VMEM((planes_i * 2, 8, 2 * rows), f32),
            pltpu.VMEM((planes_t, 8, 2 * rows), f32),
            pltpu.VMEM((planes_i * 4, 8, 2 * rows), f32),
            pltpu.VMEM((planes_t * 2, 8, 2 * rows), f32),
            dma((2,)),
            dma((2,)),
            dma((2,)),
            dma((planes_t, TEXT_CHUNKS)),
            dma((planes_i, IMAGE_CHUNKS)),
            dma((planes_t, TEXT_CHUNKS)),
            dma((planes_i, IMAGE_CHUNKS)),
            dma((planes_i, 2, IMAGE_CHUNKS)),
            dma((planes_t, 2, TEXT_CHUNKS)),
            dma((planes_i, 2, 2, IMAGE_CHUNKS)),
            dma((planes_i, 2, 2)),
            dma((planes_t, 2)),
            dma((planes_i * 4,)),
            dma((planes_t * 2,)),
        ],
        compiler_params=pltpu.CompilerParams(
            collective_id=0, has_side_effects=True, vmem_limit_bytes=VMEM_BYTES
        ),
    )(logit_scale, images, texts)
    return losses[0], losses[1]


def solution(mesh):
    planes = mesh.shape["dp"] // 4
    planes_i = max(d for d in range(1, planes + 1) if planes % d == 0 and d * d <= planes)
    in_specs = (P("dp", None), P(("dp", "outer"), None), P())
    out_specs = (P(("dp", "outer")), P(("dp", "outer")))
    return jax.shard_map(
        functools.partial(on_device, planes_i, planes // planes_i),
        mesh=mesh, in_specs=in_specs, out_specs=out_specs, check_vma=False,
    )
```
